512 devices in a mesh: unit: 2 (over y_1), row: 16 (over y_0, x, core), col: 16 (over z, y_2).
Axes of the slice: x: 4, y: 8 (y_0: 2, y_1: 2, y_2: 2; y = y_0 * 4 + y_1 * 2 + y_2), z: 8, core: 2. Of those that a mesh axis runs over, the one named last changes fastest.
Arguments:
- tracer: float32 [4, 128, 256, 256], P('unit', None, 'row', 'col'), parts along dimension 0, may hold values from -6 to 6
- symbol_x: float32 [128], replicated, may hold values from 0.3 to 3
- symbol_y: float32 [256], replicated, may hold values from 0.3 to 3
- symbol_z: float32 [256], replicated, may hold values from 0.3 to 3
Outputs:
- smoothed: float32 [4, 128, 256, 256], P('unit', None, 'row', 'col'), parts along dimension 0
The draws below stay inside these ranges and needn't reach their ends.
There are 2 independent parts, one for each index of `unit`. The reference program is written for one: setup_inputs(seed, part) draws one part's arguments, and reference() takes and returns one part's arrays. A program takes and returns all parts, laid end to end along the dimension named above; an argument that names none is the same for every part. Nothing has to cross between parts.
All inputs are finite; a program needn't handle non-finite values.
Results may differ from the reference program's by a relative error of at most 0.0003.
Values sent between devices are 32-bit elements.
A program may use at most 64 MiB of HBM per device.

```python
import jax
import jax.numpy as jnp
from jax import lax

GRID_X = 128
GRID_Y = 256
GRID_Z = 256
FIELDS = 2


def levels(stream_key, extent, shards, smallest, top_value):
    def one(dim, shards_of):
        steps = jax.random.uniform(jax.random.fold_in(jax.random.fold_in(stream_key, 6), dim), (shards_of,), jnp.float32, smallest / len(shards), top_value / len(shards))
        return jnp.repeat(jnp.exp(steps), extent[dim] // shards_of).reshape((-1,) + (1,) * (len(extent) - dim - 1))

    factor_of = one(*shards[0])
    for cut in shards[1:]:
        factor_of = factor_of * one(*cut)
    return factor_of


def noise(key, extent, deviation, bound, split=(), dtype=jnp.bfloat16):
    level = levels(key, extent, split, -0.22, 0.18) if split else 1.0
    drawn = jax.random.normal(key, extent, jnp.float32) * deviation * level
    return jnp.minimum(jnp.maximum(drawn, -bound), bound).astype(dtype)


def setup_inputs(seed: int = 0, part: int = 0) -> dict:
    arg_keys = jax.random.split(jax.random.key(seed), 5)
    part_keys = jax.random.split(jax.random.fold_in(arg_keys[4], part), 5)
    return {
        "tracer": noise(part_keys[0], (FIELDS, GRID_X, GRID_Y, GRID_Z), 1.0, 6.0, ((2, 16), (3, 16)), jnp.float32),
        "symbol_x": jnp.clip(jax.random.uniform(arg_keys[1], (GRID_X,), jnp.float32, 0.3, 3.0), 0.3, 3.0),
        "symbol_y": jnp.clip(jax.random.uniform(arg_keys[2], (GRID_Y,), jnp.float32, 0.3, 3.0), 0.3, 3.0),
        "symbol_z": jnp.clip(jax.random.uniform(arg_keys[3], (GRID_Z,), jnp.float32, 0.3, 3.0), 0.3, 3.0),
    }


def mode_table(count):
    rank = jnp.arange(count)
    angle = jnp.pi / (4 * count) * ((2 * rank[:, None] + 1) * (2 * rank[None, :] + 1) % (8 * count)).astype(jnp.float32)
    return jnp.cos(angle) * (2.0 / count) ** 0.5

def to_modes(values, dim):
    moved = jnp.tensordot(values, mode_table(values.shape[dim]), axes=([dim], [0]), precision=lax.Precision.HIGHEST)
    return jnp.moveaxis(moved, -1, dim)

def reference(tracer, symbol_x, symbol_y, symbol_z):
    modes = tracer
    modes = to_modes(modes, 1)
    modes = to_modes(modes, 2)
    modes = to_modes(modes, 3)
    symbol = symbol_x[:, None, None] + symbol_y[None, :, None] + symbol_z[None, None, :]
    modes = modes * lax.rsqrt(symbol)
    smoothed = modes
    smoothed = to_modes(smoothed, 3)
    smoothed = to_modes(smoothed, 2)
    smoothed = to_modes(smoothed, 1)
    return smoothed
```

```python
import functools

import jax
import jax.numpy as jnp
import ml_dtypes
import numpy as np
from jax import lax
from jax.experimental import pallas as pl
from jax.experimental.pallas import tpu as pltpu
from jax.sharding import PartitionSpec as P

MESH = pl.DeviceIdType.MESH
F32 = jnp.float32
BF16 = jnp.bfloat16


def cosines(count):
    rank = np.arange(count)
    angle = np.pi / (4 * count) * ((2 * rank[:, None] + 1) * (2 * rank[None, :] + 1) % (8 * count))
    return np.cos(angle) * (2.0 / count) ** 0.5


def halves(table):
    table = table.astype(np.float32)
    high = table.astype(ml_dtypes.bfloat16)
    low = (table - high.astype(np.float32)).astype(ml_dtypes.bfloat16)
    return np.stack([high, low])


def tables():
    full = cosines(256)
    h, r, i = np.meshgrid(np.arange(2), np.arange(16), np.arange(8), indexing="ij")
    rows = (r * 16 + h * 8 + i).reshape(-1)
    s, z, j = np.meshgrid(np.arange(2), np.arange(8), np.arange(16), indexing="ij")
    lanes = ((z * 2 + s) * 16 + j).reshape(-1)
    big = np.stack([halves(full[lanes, :]), halves(full[:, rows]), halves(full[rows, :]), halves(full[:, lanes])])
    return halves(cosines(128)), big


def split(value):
    high = value.astype(BF16)
    return high, (value - high.astype(F32)).astype(BF16)


def dot3(left, right, dims=(((1,), (0,)), ((), ()))):
    def dot(a, b):
        return lax.dot_general(a, b, dims, preferred_element_type=F32)

    return dot(left[0], right[0]) + (dot(left[0], right[1]) + dot(left[1], right[0]))


def swap_blocks(value):
    sub = lax.broadcasted_iota(jnp.int32, value.shape, 1)
    lane = lax.broadcasted_iota(jnp.int32, value.shape, 2) // 16
    for bit in (4, 2, 1):
        s_on = (sub // bit) % 2
        l_on = (lane // bit) % 2
        down = pltpu.roll(pltpu.roll(value, bit, 1), 128 - 16 * bit, 2)
        up = down if bit == 4 else pltpu.roll(pltpu.roll(value, 8 - bit, 1), 16 * bit, 2)
        value = jnp.where(s_on == l_on, value, jnp.where(s_on == 1, down, up))
    return value


def kernel(t_hbm, sx_hbm, sy_hbm, sz_hbm, hx_hbm, big_hbm, out_ref, *scratch):
    (t, sx, sy, sz, hx, big, scale, plane, mixed) = scratch[:9]
    m, ra, sb, rb, sb2, rb2, sa2, ra2 = (scratch[9 + 2 * k : 11 + 2 * k] for k in range(8))
    in_sem, send, recv = scratch[25:]

    r = lax.axis_index("row")
    c = lax.axis_index("col")
    core = lax.rem(r, 2)
    x0 = lax.rem(r // 2, 2)
    x1 = lax.rem(r // 4, 2)
    y0 = r // 8
    y2 = lax.rem(c, 2)
    z0 = lax.rem(c // 2, 2)
    z1 = lax.rem(c // 4, 2)
    z2 = c // 8
    alpha = lax.rem(y0 + y2, 2)
    my_a = core * 8 + x1 * 4 + x0 * 2 + alpha
    my_b = z2 * 8 + z1 * 4 + z0 * 2 + y0
    a_bits = {
        8: (1 - 2 * core, None, 8 - 16 * core),
        4: (4 - 8 * x1, None, 4 - 8 * x1),
        2: (2 - 4 * x0, None, 2 - 4 * x0),
        1: (None, 1 - 2 * y2, 1 - 2 * alpha),
    }
    b_bits = {
        8: (None, 8 - 16 * z2, 8 - 16 * z2),
        4: (None, 4 - 8 * z1, 4 - 8 * z1),
        2: (None, 2 - 4 * z0, 2 - 4 * z0),
        1: (8 - 16 * y0, 1 - 2 * y2, 1 - 2 * y0),
    }

    def peers(bits, own):
        found = {0: (r, c, own)}
        for mask in range(1, 16):
            bit = mask & -mask
            here = found[mask ^ bit]
            found[mask] = tuple(h if d is None else h + d for h, d in zip(here, bits[bit]))
        return [found[k] for k in (15, 14, 13, 12, 11, 10, 9, 8, 7, 6, 5, 4, 3, 2, 1)]

    a_peers = peers(a_bits, my_a)
    b_peers = peers(b_bits, my_b)

    barrier = pltpu.get_barrier_semaphore()
    for row, col, _ in b_peers + a_peers:
        pl.semaphore_signal(barrier, inc=1, device_id={"row": row, "col": col}, device_id_type=MESH)

    loads = [
        pltpu.make_async_copy(src, dst, in_sem.at[k])
        for k, (src, dst) in enumerate(
            [(t_hbm, t), (hx_hbm, hx), (sx_hbm, sx), (sy_hbm, sy), (sz_hbm, sz), (big_hbm, big)]
        )
    ]
    for load in loads:
        load.start()

    def copy(src, dst, stage, h, peer, own):
        row, col, place = peer
        return pltpu.make_async_remote_copy(
            src_ref=src[h].at[pl.ds(pl.multiple_of(place * 16, 16), 16)],
            dst_ref=dst[h].at[pl.ds(pl.multiple_of(own * 16, 16), 16)],
            send_sem=send.at[stage, h],
            recv_sem=recv.at[stage, h],
            device_id={"row": row, "col": col},
            device_id_type=MESH,
        )

    def start(src, dst, stage, h, group, own):
        for peer in group:
            copy(src, dst, stage, h, peer, own).start()
        mine = pl.ds(pl.multiple_of(own * 16, 16), 16)
        dst[h][mine, :] = src[h][mine, :]

    def whole(src, dst, stage, h):
        return pltpu.make_async_remote_copy(
            src_ref=src[h].at[pl.ds(0, 240)],
            dst_ref=dst[h].at[pl.ds(0, 240)],
            send_sem=send.at[stage, h],
            recv_sem=recv.at[stage, h],
            device_id={"row": r, "col": c},
            device_id_type=MESH,
        )

    def regroup(src, dst):
        for k in range(16):
            dst[16 * k : 16 * k + 16, :] = src[pl.ds(k, 16, stride=16), :]

    loads[0].wait()
    loads[1].wait()
    table_x = (hx[0], hx[1])
    for h in range(2):
        for f in range(2):
            lines = split(t[256 * f + 128 * h : 256 * f + 128 * h + 128, :])
            m[h][128 * f : 128 * f + 128, :] = dot3(table_x, lines, (((1,), (1,)), ((), ())))

    pl.semaphore_wait(barrier, 30)
    for h in range(2):
        start(m, ra, 0, h, a_peers, my_a)

    for load in loads[2:]:
        load.wait()
    mode = (x1 * 4 + x0 * 2 + alpha) * 16 + my_b
    at = lax.broadcasted_iota(jnp.int32, (1, 128), 1)
    part_x = jnp.sum(jnp.where(at == mode, sx[...], 0.0), axis=1, keepdims=True)
    for k in range(2):
        part_y = jnp.broadcast_to(sy[:, 128 * k : 128 * k + 128], (128, 128)).T
        for n in range(2):
            where = (slice(128 * k, 128 * k + 128), slice(128 * n, 128 * n + 128))
            scale[where] = lax.rsqrt(part_x + part_y + sz[:, 128 * n : 128 * n + 128])

    for h in range(2):
        whole(m, ra, 0, h).wait_recv()
        regroup(ra[h], sb[h])
        start(sb, rb, 1, h, b_peers, my_b)

    def at_of(k):
        row, s = k // 2, k % 2
        beta, x, own_core = row // 8, row // 2 % 4, row % 2
        return pl.ds(beta * 16 + own_core * 8 + x * 2 + (s ^ beta), 8, stride=32)

    part = [None, None]
    for h in range(2):
        whole(sb, rb, 1, h).wait_recv()
        tiles = swap_blocks(jnp.stack([rb[h][at_of(k), :] for k in range(32)]))
        for k in range(32):
            plane[8 * (k // 2) : 8 * (k // 2) + 8, 128 * (k % 2) : 128 * (k % 2) + 128] = tiles[k]
        lines = split(dot3(split(plane[...]), (big[0, 0], big[0, 1])))
        cols = slice(128 * h, 128 * h + 128)
        part[h] = dot3((big[1, 0, :, cols], big[1, 1, :, cols]), lines)
    mixed[...] = (part[0] + part[1]) * scale[...]
    modes = split(mixed[...])

    for h in range(2):
        rows = slice(128 * h, 128 * h + 128)
        lines = split(dot3((big[2, 0, rows, :], big[2, 1, rows, :]), modes))
        back = dot3(lines, (big[3, 0], big[3, 1]))
        tiles = swap_blocks(
            jnp.stack(
                [back[8 * (k // 2) : 8 * (k // 2) + 8, 128 * (k % 2) : 128 * (k % 2) + 128] for k in range(32)]
            )
        )
        for k in range(32):
            sb2[h][at_of(k), :] = tiles[k]
        start(sb2, rb2, 2, h, b_peers, my_b)

    for h in range(2):
        whole(sb2, rb2, 2, h).wait_recv()
        regroup(rb2[h], sa2[h])
        start(sa2, ra2, 3, h, a_peers, my_a)

    for h in range(2):
        whole(sa2, ra2, 3, h).wait_recv()
        for f in range(2):
            lines = split(ra2[h][128 * f : 128 * f + 128, :].T)
            out_ref[256 * f + 128 * h : 256 * f + 128 * h + 128, :] = dot3(lines, table_x)

    for stage, (src, dst) in enumerate(((m, ra), (sb, rb), (sb2, rb2), (sa2, ra2))):
        for h in range(2):
            whole(src, dst, stage, h).wait_send()


def shards(tracer, symbol_x, symbol_y, symbol_z):
    table_x, big = tables()
    lines = jnp.transpose(tracer, (0, 2, 3, 1)).reshape(512, 128)
    anywhere = pl.BlockSpec(memory_space=pl.ANY)
    result = pl.pallas_call(
        kernel,
        out_shape=jax.ShapeDtypeStruct((512, 128), F32),
        in_specs=[anywhere] * 6,
        out_specs=pl.BlockSpec(memory_space=pltpu.VMEM),
        scratch_shapes=[
            pltpu.VMEM((512, 128), F32),
            pltpu.VMEM((1, 128), F32),
            pltpu.VMEM((1, 256), F32),
            pltpu.VMEM((1, 256), F32),
            pltpu.VMEM((2, 128, 128), BF16),
            pltpu.VMEM((4, 2, 256, 256), BF16),
            pltpu.VMEM((256, 256), F32),
            pltpu.VMEM((128, 256), F32),
            pltpu.VMEM((256, 256), F32),
        ]
        + [pltpu.VMEM((256, 128), F32)] * 16
        + [
            pltpu.SemaphoreType.DMA((6,)),
            pltpu.SemaphoreType.DMA((4, 2)),
            pltpu.SemaphoreType.DMA((4, 2)),
        ],
        compiler_params=pltpu.CompilerParams(collective_id=0, has_side_effects=True),
    )(
        lines,
        symbol_x.reshape(1, 128),
        symbol_y.reshape(1, 256),
        symbol_z.reshape(1, 256),
        jnp.asarray(table_x),
        jnp.asarray(big),
    )
    return jnp.transpose(result.reshape(2, 16, 16, 128), (0, 3, 1, 2))


def solution(mesh):
    in_specs = (P("unit", None, "row", "col"), P(), P(), P())
    out_specs = P("unit", None, "row", "col")
    return jax.shard_map(shards, mesh=mesh, in_specs=in_specs, out_specs=out_specs, check_vma=False)
```

```python
import functools

import jax
import jax.numpy as jnp
import ml_dtypes
import numpy as np
from jax import lax
from jax.experimental import pallas as pl
from jax.experimental.pallas import tpu as pltpu
from jax.sharding import PartitionSpec as P

MESH = pl.DeviceIdType.MESH
F32 = jnp.float32
BF16 = jnp.bfloat16


def cosines(count):
    rank = np.arange(count)
    angle = np.pi / (4 * count) * ((2 * rank[:, None] + 1) * (2 * rank[None, :] + 1) % (8 * count))
    return np.cos(angle) * (2.0 / count) ** 0.5


def halves(table):
    table = table.astype(np.float32)
    high = table.astype(ml_dtypes.bfloat16)
    low = (table - high.astype(np.float32)).astype(ml_dtypes.bfloat16)
    return np.stack([high, low])


def tables():
    full = cosines(256)
    h, r, i = np.meshgrid(np.arange(2), np.arange(16), np.arange(8), indexing="ij")
    rows = (r * 16 + h * 8 + i).reshape(-1)
    s, z, j = np.meshgrid(np.arange(2), np.arange(8), np.arange(16), indexing="ij")
    lanes = ((z * 2 + s) * 16 + j).reshape(-1)
    big = np.stack([halves(full[lanes, :]), halves(full[:, rows]), halves(full[rows, :]), halves(full[:, lanes])])
    modes = cosines(128)
    return np.stack([halves(modes), halves(modes.reshape(8, 16, 128).transpose(1, 0, 2).reshape(128, 128))]), big


def split(value):
    high = value.astype(BF16)
    return high, (value - high.astype(F32)).astype(BF16)


def dot3(left, right, dims=(((1,), (0,)), ((), ()))):
    def dot(a, b):
        return lax.dot_general(a, b, dims, preferred_element_type=F32)

    return dot(left[0], right[0]) + (dot(left[0], right[1]) + dot(left[1], right[0]))


def swap_blocks(value):
    sub = lax.broadcasted_iota(jnp.int32, value.shape, 1)
    lane = lax.broadcasted_iota(jnp.int32, value.shape, 2) // 16
    for bit in (4, 2, 1):
        s_on = (sub // bit) % 2
        l_on = (lane // bit) % 2
        down = pltpu.roll(pltpu.roll(value, bit, 1), 128 - 16 * bit, 2)
        up = down if bit == 4 else pltpu.roll(pltpu.roll(value, 8 - bit, 1), 16 * bit, 2)
        value = jnp.where(s_on == l_on, value, jnp.where(s_on == 1, down, up))
    return value


def kernel(t_hbm, sx_hbm, sy_hbm, sz_hbm, hx_hbm, big_hbm, out_ref, *scratch):
    (t, sx, sy, sz, hx, big, scale, plane, mixed) = scratch[:9]
    m, first, turned, arrived, leaving, third, turned2, home = (scratch[9 + 2 * k : 11 + 2 * k] for k in range(8))
    in_sem, send, recv = scratch[25:]

    loads = [
        pltpu.make_async_copy(src, dst, in_sem.at[k])
        for k, (src, dst) in enumerate(
            [(t_hbm, t), (hx_hbm, hx), (sx_hbm, sx), (sy_hbm, sy), (sz_hbm, sz), (big_hbm, big)]
        )
    ]
    for load in loads:
        load.start()

    r = lax.axis_index("row")
    c = lax.axis_index("col")
    core = lax.rem(r, 2)
    x0 = lax.rem(r // 2, 2)
    x1 = lax.rem(r // 4, 2)
    y0 = r // 8
    y2 = lax.rem(c, 2)
    z0 = lax.rem(c // 2, 2)
    z1 = lax.rem(c // 4, 2)
    z2 = c // 8
    alpha = lax.rem(y0 + y2, 2)
    my_a = core * 8 + x1 * 4 + x0 * 2 + y0
    my_b = z2 * 8 + z1 * 4 + z0 * 2 + alpha
    a_bits = {
        8: (1 - 2 * core, None, 8 - 16 * core),
        4: (4 - 8 * x1, None, 4 - 8 * x1),
        2: (2 - 4 * x0, None, 2 - 4 * x0),
        1: (8 - 16 * y0, 1 - 2 * y2, 1 - 2 * y0),
    }
    b_bits = {
        8: (None, 8 - 16 * z2, 8 - 16 * z2),
        4: (None, 4 - 8 * z1, 4 - 8 * z1),
        2: (None, 2 - 4 * z0, 2 - 4 * z0),
        1: (None, 1 - 2 * y2, 1 - 2 * alpha),
    }

    def peers(bits, own):
        found = {0: (r, c, own)}
        for mask in range(1, 16):
            bit = mask & -mask
            here = found[mask ^ bit]
            found[mask] = tuple(h if d is None else h + d for h, d in zip(here, bits[bit]))
        return [found[k] for k in (15, 14, 13, 12, 11, 10, 9, 8, 7, 6, 5, 4, 3, 2, 1)]

    a_peers = peers(a_bits, my_a)
    b_peers = peers(b_bits, my_b)

    barrier = pltpu.get_barrier_semaphore()
    for row, col, _ in b_peers + a_peers:
        pl.semaphore_signal(barrier, inc=1, device_id={"row": row, "col": col}, device_id_type=MESH)

    def copy(src, dst, stage, h, peer, own):
        row, col, place = peer
        return pltpu.make_async_remote_copy(
            src_ref=src[h].at[pl.ds(pl.multiple_of(place * 16, 16), 16)],
            dst_ref=dst[h].at[pl.ds(pl.multiple_of(own * 16, 16), 16)],
            send_sem=send.at[stage, h],
            recv_sem=recv.at[stage, h],
            device_id={"row": row, "col": col},
            device_id_type=MESH,
        )

    def start(src, dst, stage, h, group, own):
        for peer in group:
            copy(src, dst, stage, h, peer, own).start()
        mine = pl.ds(pl.multiple_of(own * 16, 16), 16)
        dst[h][mine, :] = src[h][mine, :]

    def whole(src, dst, stage, h):
        return pltpu.make_async_remote_copy(
            src_ref=src[h].at[pl.ds(0, 240)],
            dst_ref=dst[h].at[pl.ds(0, 240)],
            send_sem=send.at[stage, h],
            recv_sem=recv.at[stage, h],
            device_id={"row": r, "col": c},
            device_id_type=MESH,
        )

    def regroup(src, dst):
        for k in range(16):
            dst[16 * k : 16 * k + 16, :] = src[pl.ds(k, 16, stride=16), :]

    groups = {"a": (a_peers, my_a), "b": (b_peers, my_b)}

    loads[0].wait()
    loads[1].wait()
    tables_x = [(hx[h, 0], hx[h, 1]) for h in range(2)]
    for h in range(2):
        for f in range(2):
            lines = split(t[256 * f + 128 * h : 256 * f + 128 * h + 128, :])
            found = dot3(tables_x[h], lines, (((1,), (1,)), ((), ())))
            if h == 0:
                m[0][128 * f : 128 * f + 128, :] = found
            else:
                for k in range(16):
                    m[1][16 * k + 8 * f : 16 * k + 8 * f + 8, :] = found[8 * k : 8 * k + 8]
        if h == 0:
            pl.semaphore_wait(barrier, 30)
        start(m, first, 0, h, *groups["ab"[h]])

    for load in loads[2:]:
        load.wait()
    mode = (x1 * 4 + x0 * 2 + y0) * 16 + my_b
    at = lax.broadcasted_iota(jnp.int32, (1, 128), 1)
    part_x = jnp.sum(jnp.where(at == mode, sx[...], 0.0), axis=1, keepdims=True)
    for k in range(2):
        part_y = jnp.broadcast_to(sy[:, 128 * k : 128 * k + 128], (128, 128)).T
        for n in range(2):
            where = (slice(128 * k, 128 * k + 128), slice(128 * n, 128 * n + 128))
            scale[where] = lax.rsqrt(part_x + part_y + sz[:, 128 * n : 128 * n + 128])

    for h in range(2):
        whole(m, first, 0, h).wait_recv()
        regroup(first[h], turned[h])
        start(turned, arrived, 1, h, *groups["ba"[h]])

    def at_of(h, k):
        row, s = k // 2, k % 2
        beta, x, own_core = row // 8, row // 2 % 4, row % 2
        a, b = own_core * 8 + x * 2 + beta, s ^ beta
        return pl.ds(b * 16 + a, 8, stride=32) if h == 0 else pl.ds(a * 16 + b, 8, stride=2)

    part = [None, None]
    for h in range(2):
        whole(turned, arrived, 1, h).wait_recv()
        tiles = swap_blocks(jnp.stack([arrived[h][at_of(h, k), :] for k in range(32)]))
        for k in range(32):
            plane[8 * (k // 2) : 8 * (k // 2) + 8, 128 * (k % 2) : 128 * (k % 2) + 128] = tiles[k]
        lines = split(dot3(split(plane[...]), (big[0, 0], big[0, 1])))
        cols = slice(128 * h, 128 * h + 128)
        part[h] = dot3((big[1, 0, :, cols], big[1, 1, :, cols]), lines)
    mixed[...] = (part[0] + part[1]) * scale[...]
    modes = split(mixed[...])

    for h in range(2):
        rows = slice(128 * h, 128 * h + 128)
        lines = split(dot3((big[2, 0, rows, :], big[2, 1, rows, :]), modes))
        back = dot3(lines, (big[3, 0], big[3, 1]))
        tiles = swap_blocks(
            jnp.stack(
                [back[8 * (k // 2) : 8 * (k // 2) + 8, 128 * (k % 2) : 128 * (k % 2) + 128] for k in range(32)]
            )
        )
        for k in range(32):
            leaving[h][at_of(h, k), :] = tiles[k]
        start(leaving, third, 2, h, *groups["ba"[h]])

    for h in range(2):
        whole(leaving, third, 2, h).wait_recv()
        regroup(third[h], turned2[h])
        start(turned2, home, 3, h, *groups["ab"[h]])

    for h in range(2):
        whole(turned2, home, 3, h).wait_recv()
        for f in range(2):
            if h == 0:
                lines = home[0][128 * f : 128 * f + 128, :]
            else:
                lines = jnp.concatenate([home[1][16 * k + 8 * f : 16 * k + 8 * f + 8, :] for k in range(16)])
            out_ref[256 * f + 128 * h : 256 * f + 128 * h + 128, :] = dot3(split(lines.T), tables_x[h])

    for stage, (src, dst) in enumerate(((m, first), (turned, arrived), (leaving, third), (turned2, home))):
        for h in range(2):
            whole(src, dst, stage, h).wait_send()


def shards(tracer, symbol_x, symbol_y, symbol_z):
    table_x, big = tables()
    lines = jnp.transpose(tracer, (0, 2, 3, 1)).reshape(512, 128)
    anywhere = pl.BlockSpec(memory_space=pl.ANY)
    result = pl.pallas_call(
        kernel,
        out_shape=jax.ShapeDtypeStruct((512, 128), F32),
        in_specs=[anywhere] * 6,
        out_specs=pl.BlockSpec(memory_space=pltpu.VMEM),
        scratch_shapes=[
            pltpu.VMEM((512, 128), F32),
            pltpu.VMEM((1, 128), F32),
            pltpu.VMEM((1, 256), F32),
            pltpu.VMEM((1, 256), F32),
            pltpu.VMEM((2, 2, 128, 128), BF16),
            pltpu.VMEM((4, 2, 256, 256), BF16),
            pltpu.VMEM((256, 256), F32),
            pltpu.VMEM((128, 256), F32),
            pltpu.VMEM((256, 256), F32),
        ]
        + [pltpu.VMEM((256, 128), F32)] * 16
        + [
            pltpu.SemaphoreType.DMA((6,)),
            pltpu.SemaphoreType.DMA((4, 2)),
            pltpu.SemaphoreType.DMA((4, 2)),
        ],
        compiler_params=pltpu.CompilerParams(collective_id=0, has_side_effects=True),
    )(
        lines,
        symbol_x.reshape(1, 128),
        symbol_y.reshape(1, 256),
        symbol_z.reshape(1, 256),
        jnp.asarray(table_x),
        jnp.asarray(big),
    )
    return jnp.transpose(result.reshape(2, 16, 16, 128), (0, 3, 1, 2))


def solution(mesh):
    in_specs = (P("unit", None, "row", "col"), P(), P(), P())
    out_specs = P("unit", None, "row", "col")
    return jax.shard_map(shards, mesh=mesh, in_specs=in_specs, out_specs=out_specs, check_vma=False)
```

```python
import functools

import jax
import jax.numpy as jnp
import ml_dtypes
import numpy as np
from jax import lax
from jax.experimental import pallas as pl
from jax.experimental.pallas import tpu as pltpu
from jax.sharding import PartitionSpec as P

MESH = pl.DeviceIdType.MESH
F32 = jnp.float32
BF16 = jnp.bfloat16


def cosines(count):
    rank = np.arange(count)
    angle = np.pi / (4 * count) * ((2 * rank[:, None] + 1) * (2 * rank[None, :] + 1) % (8 * count))
    return np.cos(angle) * (2.0 / count) ** 0.5


def halves(table):
    table = table.astype(np.float32)
    high = table.astype(ml_dtypes.bfloat16)
    low = (table - high.astype(np.float32)).astype(ml_dtypes.bfloat16)
    return np.stack([high, low])


def tables():
    full = cosines(256)
    h, r, i = np.meshgrid(np.arange(2), np.arange(16), np.arange(8), indexing="ij")
    rows = (r * 16 + h * 8 + i).reshape(-1)
    s, z, j = np.meshgrid(np.arange(2), np.arange(8), np.arange(16), indexing="ij")
    lanes = ((z * 2 + s) * 16 + j).reshape(-1)
    big = np.stack([halves(full[lanes, :]), halves(full[:, rows]), halves(full[rows, :]), halves(full[:, lanes])])
    modes = cosines(128)
    return np.stack([halves(modes), halves(modes.reshape(8, 16, 128).transpose(1, 0, 2).reshape(128, 128))]), big


def split(value):
    high = value.astype(BF16)
    return high, (value - high.astype(F32)).astype(BF16)


def dot3(left, right, dims=(((1,), (0,)), ((), ()))):
    def dot(a, b):
        return lax.dot_general(a, b, dims, preferred_element_type=F32)

    return dot(left[0], right[0]) + (dot(left[0], right[1]) + dot(left[1], right[0]))


def swap_blocks(value):
    sub = lax.broadcasted_iota(jnp.int32, value.shape, 1)
    lane = lax.broadcasted_iota(jnp.int32, value.shape, 2) // 16
    for bit in (4, 2, 1):
        s_on = (sub // bit) % 2
        l_on = (lane // bit) % 2
        down = pltpu.roll(pltpu.roll(value, bit, 1), 128 - 16 * bit, 2)
        up = down if bit == 4 else pltpu.roll(pltpu.roll(value, 8 - bit, 1), 16 * bit, 2)
        value = jnp.where(s_on == l_on, value, jnp.where(s_on == 1, down, up))
    return value


def kernel(t_hbm, sx_hbm, sy_hbm, sz_hbm, hx_hbm, big_hbm, out_ref, *scratch):
    (t, sx, sy, sz, hx, big, scale, plane, mixed) = scratch[:9]
    m, first, turned, arrived, leaving, third, turned2, home = (scratch[9 + 2 * k : 11 + 2 * k] for k in range(8))
    in_sem, send, recv = scratch[25:]

    loads = [
        pltpu.make_async_copy(src, dst, in_sem.at[k])
        for k, (src, dst) in enumerate(
            [(t_hbm, t), (hx_hbm, hx), (sx_hbm, sx), (sy_hbm, sy), (sz_hbm, sz), (big_hbm, big)]
        )
    ]
    for load in loads:
        load.start()

    r = lax.axis_index("row")
    c = lax.axis_index("col")
    core = lax.rem(r, 2)
    x0 = lax.rem(r // 2, 2)
    x1 = lax.rem(r // 4, 2)
    y0 = r // 8
    y2 = lax.rem(c, 2)
    z0 = lax.rem(c // 2, 2)
    z1 = lax.rem(c // 4, 2)
    z2 = c // 8
    alpha = lax.rem(y0 + y2, 2)
    my_a = core * 8 + x1 * 4 + x0 * 2 + y0
    my_b = z2 * 8 + z1 * 4 + z0 * 2 + alpha
    a_bits = {
        8: (1 - 2 * core, None, 8 - 16 * core),
        4: (4 - 8 * x1, None, 4 - 8 * x1),
        2: (2 - 4 * x0, None, 2 - 4 * x0),
        1: (8 - 16 * y0, 1 - 2 * y2, 1 - 2 * y0),
    }
    b_bits = {
        8: (None, 8 - 16 * z2, 8 - 16 * z2),
        4: (None, 4 - 8 * z1, 4 - 8 * z1),
        2: (None, 2 - 4 * z0, 2 - 4 * z0),
        1: (None, 1 - 2 * y2, 1 - 2 * alpha),
    }

    def peers(bits, own):
        found = {0: (r, c, own)}
        for mask in range(1, 16):
            bit = mask & -mask
            here = found[mask ^ bit]
            found[mask] = tuple(h if d is None else h + d for h, d in zip(here, bits[bit]))
        return [found[k] for k in (15, 14, 13, 12, 11, 10, 9, 8, 7, 6, 5, 4, 3, 2, 1)]

    a_peers = peers(a_bits, my_a)
    b_peers = peers(b_bits, my_b)

    barrier = pltpu.get_barrier_semaphore()
    for row, col, _ in b_peers + a_peers:
        pl.semaphore_signal(barrier, inc=1, device_id={"row": row, "col": col}, device_id_type=MESH)

    def copy(src, dst, stage, h, peer, own):
        row, col, place = peer
        return pltpu.make_async_remote_copy(
            src_ref=src[h].at[pl.ds(pl.multiple_of(place * 16, 16), 16)],
            dst_ref=dst[h].at[pl.ds(pl.multiple_of(own * 16, 16), 16)],
            send_sem=send.at[stage, h],
            recv_sem=recv.at[stage, h],
            device_id={"row": row, "col": col},
            device_id_type=MESH,
        )

    def start(src, dst, stage, h, group, own):
        for peer in group:
            copy(src, dst, stage, h, peer, own).start()
        mine = pl.ds(pl.multiple_of(own * 16, 16), 16)
        dst[h][mine, :] = src[h][mine, :]

    def whole(src, dst, stage, h):
        return pltpu.make_async_remote_copy(
            src_ref=src[h].at[pl.ds(0, 240)],
            dst_ref=dst[h].at[pl.ds(0, 240)],
            send_sem=send.at[stage, h],
            recv_sem=recv.at[stage, h],
            device_id={"row": r, "col": c},
            device_id_type=MESH,
        )

    def regroup(src, dst):
        for k in range(16):
            dst[16 * k : 16 * k + 16, :] = src[pl.ds(k, 16, stride=16), :]

    groups = {"a": (a_peers, my_a), "b": (b_peers, my_b)}

    loads[0].wait()
    loads[1].wait()
    tables_x = [(hx[h, 0], hx[h, 1]) for h in range(2)]
    for h in range(2):
        for f in range(2):
            lines = split(t[256 * f + 128 * h : 256 * f + 128 * h + 128, :])
            found = dot3(tables_x[h], lines, (((1,), (1,)), ((), ())))
            if h == 0:
                m[0][128 * f : 128 * f + 128, :] = found
            else:
                for k in range(16):
                    m[1][16 * k + 8 * f : 16 * k + 8 * f + 8, :] = found[8 * k : 8 * k + 8]
        if h == 0:
            pl.semaphore_wait(barrier, 30)
        start(m, first, 0, h, *groups["ab"[h]])

    for load in loads[2:]:
        load.wait()
    mode = (x1 * 4 + x0 * 2 + y0) * 16 + my_b
    at = lax.broadcasted_iota(jnp.int32, (1, 128), 1)
    part_x = jnp.sum(jnp.where(at == mode, sx[...], 0.0), axis=1, keepdims=True)
    for k in range(2):
        part_y = jnp.broadcast_to(sy[:, 128 * k : 128 * k + 128], (128, 128)).T
        for n in range(2):
            where = (slice(128 * k, 128 * k + 128), slice(128 * n, 128 * n + 128))
            scale[where] = lax.rsqrt(part_x + part_y + sz[:, 128 * n : 128 * n + 128])

    for h in range(2):
        whole(m, first, 0, h).wait_recv()
        regroup(first[h], turned[h])
        start(turned, arrived, 1, h, *groups["ba"[h]])

    def at_of(h, k):
        row, s = k // 2, k % 2
        beta, x, own_core = row // 8, row // 2 % 4, row % 2
        a, b = own_core * 8 + x * 2 + beta, s ^ beta
        return pl.ds(b * 16 + a, 8, stride=32) if h == 0 else pl.ds(a * 16 + b, 8, stride=2)

    part = [None, None]
    for h in range(2):
        whole(turned, arrived, 1, h).wait_recv()
        tiles = swap_blocks(jnp.stack([arrived[h][at_of(h, k), :] for k in range(32)]))
        for k in range(32):
            plane[8 * (k // 2) : 8 * (k // 2) + 8, 128 * (k % 2) : 128 * (k % 2) + 128] = tiles[k]
        lines = split(dot3(split(plane[...]), (big[0, 0], big[0, 1])))
        cols = slice(128 * h, 128 * h + 128)
        part[h] = dot3((big[1, 0, :, cols], big[1, 1, :, cols]), lines)
    mixed[...] = (part[0] + part[1]) * scale[...]
    modes = split(mixed[...])

    for h in range(2):
        rows = slice(128 * h, 128 * h + 128)
        lines = split(dot3((big[2, 0, rows, :], big[2, 1, rows, :]), modes))
        back = dot3(lines, (big[3, 0], big[3, 1]))
        tiles = swap_blocks(
            jnp.stack(
                [back[8 * (k // 2) : 8 * (k // 2) + 8, 128 * (k % 2) : 128 * (k % 2) + 128] for k in range(32)]
            )
        )
        for k in range(32):
            leaving[h][at_of(h, k), :] = tiles[k]
        start(leaving, third, 2, h, *groups["ba"[h]])

    for h in range(2):
        whole(leaving, third, 2, h).wait_recv()
        regroup(third[h], turned2[h])
        start(turned2, home, 3, h, *groups["ab"[h]])

    for h in range(2):
        whole(turned2, home, 3, h).wait_recv()
        for f in range(2):
            if h == 0:
                lines = home[0][128 * f : 128 * f + 128, :]
            else:
                lines = jnp.concatenate([home[1][16 * k + 8 * f : 16 * k + 8 * f + 8, :] for k in range(16)])
            out_ref[256 * f + 128 * h : 256 * f + 128 * h + 128, :] = dot3(split(lines.T), tables_x[h])

    for stage, (src, dst) in enumerate(((m, first), (turned, arrived), (leaving, third), (turned2, home))):
        for h in range(2):
            whole(src, dst, stage, h).wait_send()


def shards(tracer, symbol_x, symbol_y, symbol_z):
    table_x, big = tables()
    lines = jnp.transpose(tracer, (0, 2, 3, 1)).reshape(512, 128)
    anywhere = pl.BlockSpec(memory_space=pl.ANY)
    result = pl.pallas_call(
        kernel,
        out_shape=pltpu.VMEM((512, 128), F32),
        in_specs=[anywhere] * 6,
        out_specs=pl.BlockSpec(memory_space=pltpu.VMEM),
        scratch_shapes=[
            pltpu.VMEM((512, 128), F32),
            pltpu.VMEM((1, 128), F32),
            pltpu.VMEM((1, 256), F32),
            pltpu.VMEM((1, 256), F32),
            pltpu.VMEM((2, 2, 128, 128), BF16),
            pltpu.VMEM((4, 2, 256, 256), BF16),
            pltpu.VMEM((256, 256), F32),
            pltpu.VMEM((128, 256), F32),
            pltpu.VMEM((256, 256), F32),
        ]
        + [pltpu.VMEM((256, 128), F32)] * 16
        + [
            pltpu.SemaphoreType.DMA((6,)),
            pltpu.SemaphoreType.DMA((4, 2)),
            pltpu.SemaphoreType.DMA((4, 2)),
        ],
        compiler_params=pltpu.CompilerParams(collective_id=0, has_side_effects=True),
    )(
        lines,
        symbol_x.reshape(1, 128),
        symbol_y.reshape(1, 256),
        symbol_z.reshape(1, 256),
        jnp.asarray(table_x),
        jnp.asarray(big),
    )
    return jnp.transpose(result.reshape(2, 16, 16, 128), (0, 3, 1, 2))


def solution(mesh):
    in_specs = (P("unit", None, "row", "col"), P(), P(), P())
    out_specs = P("unit", None, "row", "col")
    return jax.shard_map(shards, mesh=mesh, in_specs=in_specs, out_specs=out_specs, check_vma=False)
```

```python
import functools

import jax
import jax.numpy as jnp
import ml_dtypes
import numpy as np
from jax import lax
from jax.experimental import pallas as pl
from jax.experimental.pallas import tpu as pltpu
from jax.sharding import PartitionSpec as P

MESH = pl.DeviceIdType.MESH
F32 = jnp.float32
BF16 = jnp.bfloat16


def cosines(count):
    rank = np.arange(count)
    angle = np.pi / (4 * count) * ((2 * rank[:, None] + 1) * (2 * rank[None, :] + 1) % (8 * count))
    return np.cos(angle) * (2.0 / count) ** 0.5


def halves(table):
    table = table.astype(np.float32)
    high = table.astype(ml_dtypes.bfloat16)
    low = (table - high.astype(np.float32)).astype(ml_dtypes.bfloat16)
    return np.stack([high, low])


def tables():
    full = cosines(256)
    h, r, i = np.meshgrid(np.arange(2), np.arange(16), np.arange(8), indexing="ij")
    rows = (r * 16 + h * 8 + i).reshape(-1)
    s, z, j = np.meshgrid(np.arange(2), np.arange(8), np.arange(16), indexing="ij")
    lanes = ((z * 2 + s) * 16 + j).reshape(-1)
    big = np.stack([halves(full[lanes, :]), halves(full[:, rows]), halves(full[rows, :]), halves(full[:, lanes])])
    modes = cosines(128)
    return np.stack([halves(modes), halves(modes.reshape(8, 16, 128).transpose(1, 0, 2).reshape(128, 128))]), big


def split(value):
    high = value.astype(BF16)
    return high, (value - high.astype(F32)).astype(BF16)


def dot3(left, right, dims=(((1,), (0,)), ((), ()))):
    (l_dim,), (r_dim,) = dims[0]
    left = jnp.concatenate([left[0], left[0], left[1]], axis=l_dim)
    right = jnp.concatenate([right[0], right[1], right[0]], axis=r_dim)
    return lax.dot_general(left, right, dims, preferred_element_type=F32)


def swap_blocks(value):
    sub = lax.broadcasted_iota(jnp.int32, value.shape, 1)
    lane = lax.broadcasted_iota(jnp.int32, value.shape, 2) // 16
    for bit in (4, 2, 1):
        s_on = (sub // bit) % 2
        l_on = (lane // bit) % 2
        down = pltpu.roll(pltpu.roll(value, bit, 1), 128 - 16 * bit, 2)
        up = down if bit == 4 else pltpu.roll(pltpu.roll(value, 8 - bit, 1), 16 * bit, 2)
        value = jnp.where(s_on == l_on, value, jnp.where(s_on == 1, down, up))
    return value


def kernel(t_hbm, sx_hbm, sy_hbm, sz_hbm, hx_hbm, big_hbm, out_ref, *scratch):
    (t, sx, sy, sz, hx, big, scale, plane, mixed) = scratch[:9]
    m, first, turned, arrived, leaving, third, turned2, home = (scratch[9 + 2 * k : 11 + 2 * k] for k in range(8))
    in_sem, send, recv = scratch[25:]

    loads = [
        pltpu.make_async_copy(src, dst, in_sem.at[k])
        for k, (src, dst) in enumerate(
            [(t_hbm, t), (hx_hbm, hx), (sx_hbm, sx), (sy_hbm, sy), (sz_hbm, sz), (big_hbm, big)]
        )
    ]
    for load in loads:
        load.start()

    r = lax.axis_index("row")
    c = lax.axis_index("col")
    core = lax.rem(r, 2)
    x0 = lax.rem(r // 2, 2)
    x1 = lax.rem(r // 4, 2)
    y0 = r // 8
    y2 = lax.rem(c, 2)
    z0 = lax.rem(c // 2, 2)
    z1 = lax.rem(c // 4, 2)
    z2 = c // 8
    alpha = lax.rem(y0 + y2, 2)
    my_a = core * 8 + x1 * 4 + x0 * 2 + y0
    my_b = z2 * 8 + z1 * 4 + z0 * 2 + alpha
    a_bits = {
        8: (1 - 2 * core, None, 8 - 16 * core),
        4: (4 - 8 * x1, None, 4 - 8 * x1),
        2: (2 - 4 * x0, None, 2 - 4 * x0),
        1: (8 - 16 * y0, 1 - 2 * y2, 1 - 2 * y0),
    }
    b_bits = {
        8: (None, 8 - 16 * z2, 8 - 16 * z2),
        4: (None, 4 - 8 * z1, 4 - 8 * z1),
        2: (None, 2 - 4 * z0, 2 - 4 * z0),
        1: (None, 1 - 2 * y2, 1 - 2 * alpha),
    }

    def peers(bits, own, order):
        found = {0: (r, c, own)}
        for mask in range(1, 16):
            bit = mask & -mask
            here = found[mask ^ bit]
            found[mask] = tuple(h if d is None else h + d for h, d in zip(here, bits[bit]))
        return [found[k] for k in order]

    a_peers = peers(a_bits, my_a, range(15, 0, -1))
    b_peers = peers(b_bits, my_b, (9, 10, 8, 11, 7, 12, 6, 13, 5, 14, 4, 15, 3, 2, 1))

    barrier = pltpu.get_barrier_semaphore()
    for row, col, _ in b_peers + a_peers:
        pl.semaphore_signal(barrier, inc=1, device_id={"row": row, "col": col}, device_id_type=MESH)

    def copy(src, dst, stage, h, peer, own):
        row, col, place = peer
        return pltpu.make_async_remote_copy(
            src_ref=src[h].at[pl.ds(pl.multiple_of(place * 16, 16), 16)],
            dst_ref=dst[h].at[pl.ds(pl.multiple_of(own * 16, 16), 16)],
            send_sem=send.at[stage, h],
            recv_sem=recv.at[stage, h],
            device_id={"row": row, "col": col},
            device_id_type=MESH,
        )

    def start(src, dst, stage, h, group, own):
        for peer in group:
            copy(src, dst, stage, h, peer, own).start()
        mine = pl.ds(pl.multiple_of(own * 16, 16), 16)
        dst[h][mine, :] = src[h][mine, :]

    def whole(src, dst, stage, h):
        return pltpu.make_async_remote_copy(
            src_ref=src[h].at[pl.ds(0, 240)],
            dst_ref=dst[h].at[pl.ds(0, 240)],
            send_sem=send.at[stage, h],
            recv_sem=recv.at[stage, h],
            device_id={"row": r, "col": c},
            device_id_type=MESH,
        )

    def regroup(src, dst):
        for k in range(16):
            dst[16 * k : 16 * k + 16, :] = src[pl.ds(k, 16, stride=16), :]

    groups = {"a": (a_peers, my_a), "b": (b_peers, my_b)}

    loads[0].wait()
    loads[1].wait()
    tables_x = [(hx[h, 0], hx[h, 1]) for h in range(2)]
    for h in range(2):
        for f in range(2):
            lines = split(t[256 * f + 128 * h : 256 * f + 128 * h + 128, :])
            found = dot3(tables_x[h], lines, (((1,), (1,)), ((), ())))
            if h == 0:
                m[0][128 * f : 128 * f + 128, :] = found
            else:
                for k in range(16):
                    m[1][16 * k + 8 * f : 16 * k + 8 * f + 8, :] = found[8 * k : 8 * k + 8]
        if h == 0:
            pl.semaphore_wait(barrier, 30)
        start(m, first, 0, h, *groups["ab"[h]])

    for load in loads[2:]:
        load.wait()
    mode = (x1 * 4 + x0 * 2 + y0) * 16 + my_b
    at = lax.broadcasted_iota(jnp.int32, (1, 128), 1)
    part_x = jnp.sum(jnp.where(at == mode, sx[...], 0.0), axis=1, keepdims=True)
    for k in range(2):
        part_y = jnp.broadcast_to(sy[:, 128 * k : 128 * k + 128], (128, 128)).T
        for n in range(2):
            where = (slice(128 * k, 128 * k + 128), slice(128 * n, 128 * n + 128))
            scale[where] = lax.rsqrt(part_x + part_y + sz[:, 128 * n : 128 * n + 128])

    for h in range(2):
        whole(m, first, 0, h).wait_recv()
        regroup(first[h], turned[h])
        start(turned, arrived, 1, h, *groups["ba"[h]])

    def at_of(h, k):
        row, s = k // 2, k % 2
        beta, x, own_core = row // 8, row // 2 % 4, row % 2
        a, b = own_core * 8 + x * 2 + beta, s ^ beta
        return pl.ds(b * 16 + a, 8, stride=32) if h == 0 else pl.ds(a * 16 + b, 8, stride=2)

    part = [None, None]
    for h in range(2):
        whole(turned, arrived, 1, h).wait_recv()
        tiles = swap_blocks(jnp.stack([arrived[h][at_of(h, k), :] for k in range(32)]))
        for k in range(32):
            plane[8 * (k // 2) : 8 * (k // 2) + 8, 128 * (k % 2) : 128 * (k % 2) + 128] = tiles[k]
        lines = split(dot3(split(plane[...]), (big[0, 0], big[0, 1])))
        cols = slice(128 * h, 128 * h + 128)
        part[h] = dot3((big[1, 0, :, cols], big[1, 1, :, cols]), lines)
    mixed[...] = (part[0] + part[1]) * scale[...]
    modes = split(mixed[...])

    for h in range(2):
        rows = slice(128 * h, 128 * h + 128)
        lines = split(dot3((big[2, 0, rows, :], big[2, 1, rows, :]), modes))
        back = dot3(lines, (big[3, 0], big[3, 1]))
        tiles = swap_blocks(
            jnp.stack(
                [back[8 * (k // 2) : 8 * (k // 2) + 8, 128 * (k % 2) : 128 * (k % 2) + 128] for k in range(32)]
            )
        )
        for k in range(32):
            leaving[h][at_of(h, k), :] = tiles[k]
        start(leaving, third, 2, h, *groups["ba"[h]])

    for h in range(2):
        whole(leaving, third, 2, h).wait_recv()
        regroup(third[h], turned2[h])
        start(turned2, home, 3, h, *groups["ab"[h]])

    for h in range(2):
        whole(turned2, home, 3, h).wait_recv()
        for f in range(2):
            if h == 0:
                lines = home[0][128 * f : 128 * f + 128, :]
            else:
                lines = jnp.concatenate([home[1][16 * k + 8 * f : 16 * k + 8 * f + 8, :] for k in range(16)])
            out_ref[256 * f + 128 * h : 256 * f + 128 * h + 128, :] = dot3(split(lines.T), tables_x[h])

    for stage, (src, dst) in enumerate(((m, first), (turned, arrived), (leaving, third), (turned2, home))):
        for h in range(2):
            whole(src, dst, stage, h).wait_send()


def shards(tracer, symbol_x, symbol_y, symbol_z):
    table_x, big = tables()
    lines = jnp.transpose(tracer, (0, 2, 3, 1)).reshape(512, 128)
    anywhere = pl.BlockSpec(memory_space=pl.ANY)
    result = pl.pallas_call(
        kernel,
        out_shape=pltpu.VMEM((512, 128), F32),
        in_specs=[anywhere] * 6,
        out_specs=pl.BlockSpec(memory_space=pltpu.VMEM),
        scratch_shapes=[
            pltpu.VMEM((512, 128), F32),
            pltpu.VMEM((1, 128), F32),
            pltpu.VMEM((1, 256), F32),
            pltpu.VMEM((1, 256), F32),
            pltpu.VMEM((2, 2, 128, 128), BF16),
            pltpu.VMEM((4, 2, 256, 256), BF16),
            pltpu.VMEM((256, 256), F32),
            pltpu.VMEM((128, 256), F32),
            pltpu.VMEM((256, 256), F32),
        ]
        + [pltpu.VMEM((256, 128), F32)] * 16
        + [
            pltpu.SemaphoreType.DMA((6,)),
            pltpu.SemaphoreType.DMA((4, 2)),
            pltpu.SemaphoreType.DMA((4, 2)),
        ],
        compiler_params=pltpu.CompilerParams(collective_id=0, has_side_effects=True),
    )(
        lines,
        symbol_x.reshape(1, 128),
        symbol_y.reshape(1, 256),
        symbol_z.reshape(1, 256),
        jnp.asarray(table_x),
        jnp.asarray(big),
    )
    return jnp.transpose(result.reshape(2, 16, 16, 128), (0, 3, 1, 2))


def solution(mesh):
    in_specs = (P("unit", None, "row", "col"), P(), P(), P())
    out_specs = P("unit", None, "row", "col")
    return jax.shard_map(shards, mesh=mesh, in_specs=in_specs, out_specs=out_specs, check_vma=False)
```

```python
import functools

import jax
import jax.numpy as jnp
import ml_dtypes
import numpy as np
from jax import lax
from jax.experimental import pallas as pl
from jax.experimental.pallas import tpu as pltpu
from jax.sharding import PartitionSpec as P

MESH = pl.DeviceIdType.MESH
F32 = jnp.float32
BF16 = jnp.bfloat16


def cosines(count):
    rank = np.arange(count)
    angle = np.pi / (4 * count) * ((2 * rank[:, None] + 1) * (2 * rank[None, :] + 1) % (8 * count))
    return np.cos(angle) * (2.0 / count) ** 0.5


def halves(table):
    table = table.astype(np.float32)
    high = table.astype(ml_dtypes.bfloat16)
    low = (table - high.astype(np.float32)).astype(ml_dtypes.bfloat16)
    return np.stack([high, low])


def tables():
    full = cosines(256)
    h, r, i = np.meshgrid(np.arange(2), np.arange(16), np.arange(8), indexing="ij")
    rows = (r * 16 + h * 8 + i).reshape(-1)
    s, z, j = np.meshgrid(np.arange(2), np.arange(8), np.arange(16), indexing="ij")
    lanes = ((z * 2 + s) * 16 + j).reshape(-1)
    big = np.stack([halves(full[lanes, :]), halves(full[:, rows]), halves(full[rows, :]), halves(full[:, lanes])])
    modes = cosines(128)
    return np.stack([halves(modes), halves(modes.reshape(8, 16, 128).transpose(1, 0, 2).reshape(128, 128))]), big


def split(value):
    high = value.astype(BF16)
    return high, (value - high.astype(F32)).astype(BF16)


def dot3(left, right, dims=(((1,), (0,)), ((), ()))):
    (l_dim,), (r_dim,) = dims[0]
    left = jnp.concatenate([left[0], left[0], left[1]], axis=l_dim)
    right = jnp.concatenate([right[0], right[1], right[0]], axis=r_dim)
    return lax.dot_general(left, right, dims, preferred_element_type=F32)


def swap_blocks(value):
    sub = lax.broadcasted_iota(jnp.int32, value.shape, 1)
    lane = lax.broadcasted_iota(jnp.int32, value.shape, 2) // 16
    for bit in (4, 2, 1):
        s_on = (sub // bit) % 2
        l_on = (lane // bit) % 2
        down = pltpu.roll(pltpu.roll(value, bit, 1), 128 - 16 * bit, 2)
        up = down if bit == 4 else pltpu.roll(pltpu.roll(value, 8 - bit, 1), 16 * bit, 2)
        value = jnp.where(s_on == l_on, value, jnp.where(s_on == 1, down, up))
    return value


def kernel(t_hbm, sx_hbm, sy_hbm, sz_hbm, hx_hbm, big_hbm, out_ref, *scratch):
    (t, sx, sy, sz, hx, big, scale, plane) = scratch[:8]
    m, first, turned, arrived, leaving, third, turned2, home = (scratch[8 + 2 * k : 10 + 2 * k] for k in range(8))
    in_sem, send, recv = scratch[24:]

    loads = [
        pltpu.make_async_copy(src, dst, in_sem.at[k])
        for k, (src, dst) in enumerate(
            [(t_hbm, t), (hx_hbm, hx), (sx_hbm, sx), (sy_hbm, sy), (sz_hbm, sz), (big_hbm, big)]
        )
    ]
    for load in loads:
        load.start()

    r = lax.axis_index("row")
    c = lax.axis_index("col")
    core = lax.rem(r, 2)
    x0 = lax.rem(r // 2, 2)
    x1 = lax.rem(r // 4, 2)
    y0 = r // 8
    y2 = lax.rem(c, 2)
    z0 = lax.rem(c // 2, 2)
    z1 = lax.rem(c // 4, 2)
    z2 = c // 8
    alpha = lax.rem(y0 + y2, 2)
    my_a = core * 8 + x1 * 4 + x0 * 2 + y0
    my_b = z2 * 8 + z1 * 4 + z0 * 2 + alpha
    a_bits = {
        8: (1 - 2 * core, None, 8 - 16 * core),
        4: (4 - 8 * x1, None, 4 - 8 * x1),
        2: (2 - 4 * x0, None, 2 - 4 * x0),
        1: (8 - 16 * y0, 1 - 2 * y2, 1 - 2 * y0),
    }
    b_bits = {
        8: (None, 8 - 16 * z2, 8 - 16 * z2),
        4: (None, 4 - 8 * z1, 4 - 8 * z1),
        2: (None, 2 - 4 * z0, 2 - 4 * z0),
        1: (None, 1 - 2 * y2, 1 - 2 * alpha),
    }

    def peers(bits, own, order):
        found = {0: (r, c, own)}
        for mask in range(1, 16):
            bit = mask & -mask
            here = found[mask ^ bit]
            found[mask] = tuple(h if d is None else h + d for h, d in zip(here, bits[bit]))
        return [found[k] for k in order]

    a_peers = peers(a_bits, my_a, range(15, 0, -1))
    b_peers = peers(b_bits, my_b, (9, 10, 8, 11, 7, 12, 6, 13, 5, 14, 4, 15, 3, 2, 1))

    barrier = pltpu.get_barrier_semaphore()
    for row, col, _ in b_peers + a_peers:
        pl.semaphore_signal(barrier, inc=1, device_id={"row": row, "col": col}, device_id_type=MESH)

    def copy(src, dst, stage, h, peer, own):
        row, col, place = peer
        return pltpu.make_async_remote_copy(
            src_ref=src[h].at[pl.ds(pl.multiple_of(place * 16, 16), 16)],
            dst_ref=dst[h].at[pl.ds(pl.multiple_of(own * 16, 16), 16)],
            send_sem=send.at[stage, h],
            recv_sem=recv.at[stage, h],
            device_id={"row": row, "col": col},
            device_id_type=MESH,
        )

    def start(src, dst, stage, h, group, own):
        for peer in group:
            copy(src, dst, stage, h, peer, own).start()
        mine = pl.ds(pl.multiple_of(own * 16, 16), 16)
        dst[h][mine, :] = src[h][mine, :]

    def whole(src, dst, stage, h):
        return pltpu.make_async_remote_copy(
            src_ref=src[h].at[pl.ds(0, 240)],
            dst_ref=dst[h].at[pl.ds(0, 240)],
            send_sem=send.at[stage, h],
            recv_sem=recv.at[stage, h],
            device_id={"row": r, "col": c},
            device_id_type=MESH,
        )

    def regroup(src, dst):
        for k in range(16):
            dst[16 * k : 16 * k + 16, :] = src[pl.ds(k, 16, stride=16), :]

    groups = {"a": (a_peers, my_a), "b": (b_peers, my_b)}

    loads[0].wait()
    loads[1].wait()
    tables_x = [(hx[h, 0], hx[h, 1]) for h in range(2)]
    for h in range(2):
        for f in range(2):
            lines = split(t[256 * f + 128 * h : 256 * f + 128 * h + 128, :])
            found = dot3(tables_x[h], lines, (((1,), (1,)), ((), ())))
            if h == 0:
                m[0][128 * f : 128 * f + 128, :] = found
            else:
                for k in range(16):
                    m[1][16 * k + 8 * f : 16 * k + 8 * f + 8, :] = found[8 * k : 8 * k + 8]
        if h == 0:
            pl.semaphore_wait(barrier, 30)
        start(m, first, 0, h, *groups["ab"[h]])

    for load in loads[2:]:
        load.wait()
    mode = (x1 * 4 + x0 * 2 + y0) * 16 + my_b
    at = lax.broadcasted_iota(jnp.int32, (1, 128), 1)
    part_x = jnp.sum(jnp.where(at == mode, sx[...], 0.0), axis=1, keepdims=True)
    for k in range(2):
        part_y = jnp.broadcast_to(sy[:, 128 * k : 128 * k + 128], (128, 128)).T
        for n in range(2):
            where = (slice(128 * k, 128 * k + 128), slice(128 * n, 128 * n + 128))
            scale[where] = lax.rsqrt(part_x + part_y + sz[:, 128 * n : 128 * n + 128])

    for h in range(2):
        whole(m, first, 0, h).wait_recv()
        regroup(first[h], turned[h])
        start(turned, arrived, 1, h, *groups["ba"[h]])

    def at_of(h, k):
        row, s = k // 2, k % 2
        beta, x, own_core = row // 8, row // 2 % 4, row % 2
        a, b = own_core * 8 + x * 2 + beta, s ^ beta
        return pl.ds(b * 16 + a, 8, stride=32) if h == 0 else pl.ds(a * 16 + b, 8, stride=2)

    part = [None, None]
    for h in range(2):
        whole(turned, arrived, 1, h).wait_recv()
        tiles = swap_blocks(jnp.stack([arrived[h][at_of(h, k), :] for k in range(32)]))
        for k in range(32):
            plane[8 * (k // 2) : 8 * (k // 2) + 8, 128 * (k % 2) : 128 * (k % 2) + 128] = tiles[k]
        lines = split(dot3(split(plane[...]), (big[0, 0], big[0, 1])))
        cols = slice(128 * h, 128 * h + 128)
        part[h] = dot3((big[1, 0, :, cols], big[1, 1, :, cols]), lines)
    modes = split((part[0] + part[1]) * scale[...])

    for h in range(2):
        rows = slice(128 * h, 128 * h + 128)
        lines = split(dot3((big[2, 0, rows, :], big[2, 1, rows, :]), modes))
        back = dot3(lines, (big[3, 0], big[3, 1]))
        tiles = swap_blocks(
            jnp.stack(
                [back[8 * (k // 2) : 8 * (k // 2) + 8, 128 * (k % 2) : 128 * (k % 2) + 128] for k in range(32)]
            )
        )
        for k in range(32):
            leaving[h][at_of(h, k), :] = tiles[k]
        start(leaving, third, 2, h, *groups["ba"[h]])

    for h in range(2):
        whole(leaving, third, 2, h).wait_recv()
        regroup(third[h], turned2[h])
        start(turned2, home, 3, h, *groups["ab"[h]])

    for h in range(2):
        whole(turned2, home, 3, h).wait_recv()
        for f in range(2):
            if h == 0:
                lines = home[0][128 * f : 128 * f + 128, :]
            else:
                lines = jnp.concatenate([home[1][16 * k + 8 * f : 16 * k + 8 * f + 8, :] for k in range(16)])
            out_ref[256 * f + 128 * h : 256 * f + 128 * h + 128, :] = dot3(split(lines.T), tables_x[h])

    for stage, (src, dst) in enumerate(((m, first), (turned, arrived), (leaving, third), (turned2, home))):
        for h in range(2):
            whole(src, dst, stage, h).wait_send()


def shards(tracer, symbol_x, symbol_y, symbol_z):
    table_x, big = tables()
    lines = jnp.transpose(tracer, (0, 2, 3, 1)).reshape(512, 128)
    anywhere = pl.BlockSpec(memory_space=pl.ANY)
    result = pl.pallas_call(
        kernel,
        out_shape=pltpu.VMEM((512, 128), F32),
        in_specs=[anywhere] * 6,
        out_specs=pl.BlockSpec(memory_space=pltpu.VMEM),
        scratch_shapes=[
            pltpu.VMEM((512, 128), F32),
            pltpu.VMEM((1, 128), F32),
            pltpu.VMEM((1, 256), F32),
            pltpu.VMEM((1, 256), F32),
            pltpu.VMEM((2, 2, 128, 128), BF16),
            pltpu.VMEM((4, 2, 256, 256), BF16),
            pltpu.VMEM((256, 256), F32),
            pltpu.VMEM((128, 256), F32),
        ]
        + [pltpu.VMEM((256, 128), F32)] * 16
        + [
            pltpu.SemaphoreType.DMA((6,)),
            pltpu.SemaphoreType.DMA((4, 2)),
            pltpu.SemaphoreType.DMA((4, 2)),
        ],
        compiler_params=pltpu.CompilerParams(collective_id=0, has_side_effects=True),
    )(
        lines,
        symbol_x.reshape(1, 128),
        symbol_y.reshape(1, 256),
        symbol_z.reshape(1, 256),
        jnp.asarray(table_x),
        jnp.asarray(big),
    )
    return jnp.transpose(result.reshape(2, 16, 16, 128), (0, 3, 1, 2))


def solution(mesh):
    in_specs = (P("unit", None, "row", "col"), P(), P(), P())
    out_specs = P("unit", None, "row", "col")
    return jax.shard_map(shards, mesh=mesh, in_specs=in_specs, out_specs=out_specs, check_vma=False)
```
